32 devices in a mesh: dp: 2 (over x), vocab: 16 (over z, y, core).
Axes of the slice: x: 2, y: 2, z: 4, core: 2. Of those that a mesh axis runs over, the one named last changes fastest.
Arguments:
- hidden: bfloat16 [512, 2304], P(('dp', 'vocab')), may hold values from -6 to 6
- targets: int32 [512], P('dp'), may hold values from 0 to 32767
- loss_weight: float32 [512], P('dp'), may hold values from 0.5 to 2
- head_weight: bfloat16 [2304, 32768], P('dp', 'vocab'), may hold values from -2.4 to 2.4
- gate_weight: bfloat16 [2304, 9216], P('dp', 'vocab'), may hold values from -0.125 to 0.125
- up_weight: bfloat16 [2304, 9216], P('dp', 'vocab'), may hold values from -0.125 to 0.125
- down_trans: bfloat16 [2304, 9216], P('dp', 'vocab'), may hold values from -0.0625 to 0.0625
- block_input: bfloat16 [384, 2304], P(('dp', 'vocab')), may hold values from -6 to 6
- block_cotangent: bfloat16 [384, 2304], P(('dp', 'vocab')), may hold values from -6 to 6
Outputs:
- token_loss: float32 [512], P('dp')
- hidden_grad: bfloat16 [512, 2304], P(('dp', 'vocab'))
- block_grad: bfloat16 [384, 2304], P(('dp', 'vocab'))
The draws below stay inside these ranges and needn't reach their ends.
All inputs are finite; a program needn't handle non-finite values.
Results may differ from the reference program's by a relative error of at most 0.012.
Values may be sent and summed in bfloat16 or wider, within the bound.
A program may use at most 128 MiB of HBM per device.

```python
import math
import jax
import jax.numpy as jnp
from jax import lax

D = 2304
FF = 9216
TOK_DEV = 256
VOCAB = 32768
TOKENS = 512
TOKENS_B = 384
N_DP = 2


def draw_hidden(key, part):
    normal_key, scale_key = jax.random.split(key, 2)
    base = jax.random.truncated_normal(normal_key, -6.0, 6.0, (TOKENS, D), jnp.float32)
    scale = jnp.exp(jax.random.uniform(scale_key, (TOKENS, 1), jnp.float32, jnp.log(1.0), jnp.log(4.0)))
    return (0.25 * base * scale).astype(jnp.bfloat16)


def draw_head_weight(key, part):
    normal_key, scale_key = jax.random.split(key, 2)
    base = jax.random.truncated_normal(normal_key, -6.0, 6.0, (D, VOCAB), jnp.float32)
    scale = jnp.exp(jax.random.uniform(scale_key, (1, VOCAB), jnp.float32, jnp.log(0.6), jnp.log(1.6)))
    return (0.25 * base * scale).astype(jnp.bfloat16)


def place_ends(array, own_key, low, top_value):
    place = [jax.random.randint(jax.random.fold_in(own_key, axis), (), 0, length) for axis, length in enumerate(array.shape)]
    main_axis = array.shape.index(max(array.shape))
    beside = place[:main_axis] + [(place[main_axis] + 1) % array.shape[main_axis]] + place[main_axis + 1:]
    return array.at[tuple(place)].set(low).at[tuple(beside)].set(top_value)


def block_scale(rng, shape, cuts, low, largest):
    loudness = 1.0
    for dim, shards_of in cuts:
        heights = jax.random.uniform(jax.random.fold_in(jax.random.fold_in(rng, 6), dim), (shards_of,), jnp.float32, low / len(cuts), largest / len(cuts))
        loudness = loudness * jnp.repeat(jnp.exp(heights), shape[dim] // shards_of).reshape((-1,) + (1,) * (len(shape) - 1 - dim))
    return loudness


def noise(stream_key, shape, spread, most, shards=(), kind=jnp.bfloat16):
    factor_of = block_scale(stream_key, shape, shards, -0.22, 0.18) if shards else 1.0
    values = jax.random.normal(stream_key, shape, jnp.float32) * spread * factor_of
    return jnp.minimum(jnp.maximum(values, -most), most).astype(kind)


def setup_inputs(seed: int = 0) -> dict:
    arg_keys = jax.random.split(jax.random.key(seed), 10)
    hidden = draw_hidden(jax.random.fold_in(arg_keys[9], 71), 0)
    targets = place_ends(jax.random.randint(arg_keys[1], (TOKENS,), 0, VOCAB), jax.random.fold_in(arg_keys[1], 1), 0, VOCAB - 1).astype(jnp.int32)
    loss_weight = jnp.clip(jnp.exp(math.log(2.0) - 1.3862944 * jax.random.uniform(arg_keys[2], (TOKENS,), jnp.float32) ** block_scale(arg_keys[2], (TOKENS,), ((0, 2),), -0.2, 0.2)), 0.5, 2.0)
    head_weight = draw_head_weight(jax.random.fold_in(arg_keys[9], 71), 0)
    gate_weight = noise(arg_keys[4], (D, FF), D ** -0.5, 0.125, ((0, 2), (1, 16)))
    up_weight = noise(arg_keys[5], (D, FF), D ** -0.5, 0.125, ((0, 2), (1, 16)))
    down_trans = noise(arg_keys[6], (D, FF), FF ** -0.5, 0.0625, ((0, 2), (1, 16)))
    block_input = noise(arg_keys[7], (TOKENS_B, D), 1.0, 6.0, ((0, 32),))
    block_cotangent = noise(arg_keys[8], (TOKENS_B, D), 1.0, 6.0, ((0, 32),))
    return dict(hidden=hidden, targets=targets, loss_weight=loss_weight, head_weight=head_weight, gate_weight=gate_weight, up_weight=up_weight, down_trans=down_trans, block_input=block_input, block_cotangent=block_cotangent)


SOFTCAP = 30.0
GELU_SCALE = 0.7978845608028654
GELU_CUBIC = 0.044715


def gelu_parts(preact):
    inner_arg = GELU_SCALE * (preact + GELU_CUBIC * preact * preact * preact)
    squash = jnp.tanh(inner_arg)
    gelu_value = 0.5 * preact * (1.0 + squash)
    derive = 0.5 * (1.0 + squash) + 0.5 * preact * (1.0 - squash * squash) * GELU_SCALE * (1.0 + 3.0 * GELU_CUBIC * preact * preact)
    return gelu_value, derive


def right_product(operand, weight):
    return lax.dot_general(operand, weight, (((1,), (1,)), ((), ())), preferred_element_type=jnp.float32)


def reference(hidden, targets, loss_weight, head_weight, gate_weight, up_weight, down_trans, block_input, block_cotangent):
    def head_group(group_args):
        group_rows, group_targets, group_weights = group_args
        logits = jnp.dot(group_rows, head_weight, preferred_element_type=jnp.float32)
        squash = jnp.tanh(logits / SOFTCAP)
        capped = SOFTCAP * squash
        cap_slope = 1.0 - squash * squash
        exponent = jnp.exp(capped)
        columns = lax.broadcasted_iota(jnp.int32, logits.shape, 1)
        target_mask = columns == group_targets[:, None]
        exp_total = jnp.sum(exponent, axis=1)
        target_logit = jnp.sum(jnp.where(target_mask, capped, 0.0), axis=1)
        group_loss = jnp.log(exp_total) - target_logit
        onehot = jnp.where(target_mask, 1.0, 0.0).astype(exponent.dtype)
        logit_cot = (group_weights[:, None] * (exponent / exp_total[:, None] - onehot) * cap_slope).astype(jnp.bfloat16)
        group_grad = right_product(logit_cot, head_weight).astype(jnp.bfloat16)
        return group_loss, group_grad

    grouped = (hidden.reshape(N_DP, TOK_DEV, D), targets.reshape(N_DP, TOK_DEV), loss_weight.reshape(N_DP, TOK_DEV))
    group_loss, group_grad = lax.map(head_group, grouped)
    token_loss = group_loss.reshape(N_DP * TOK_DEV)
    hidden_grad = group_grad.reshape(N_DP * TOK_DEV, D)

    gate_pre = jnp.dot(block_input, gate_weight, preferred_element_type=jnp.float32)
    up_pre = jnp.dot(block_input, up_weight, preferred_element_type=jnp.float32)
    hidden_cot = jnp.dot(block_cotangent, down_trans, preferred_element_type=jnp.float32)
    gate_act, derive = gelu_parts(gate_pre)
    gate_cot = (hidden_cot * up_pre * derive).astype(jnp.bfloat16)
    up_cot = (hidden_cot * gate_act).astype(jnp.bfloat16)
    block_grad = (right_product(gate_cot, gate_weight) + right_product(up_cot, up_weight)).astype(jnp.bfloat16)
    return token_loss, hidden_grad, block_grad
```

```python
import functools

import jax
import jax.numpy as jnp
from jax import lax
from jax.experimental import pallas as pl
from jax.experimental.pallas import tpu as pltpu
from jax.sharding import PartitionSpec as P

SOFTCAP = 30.0
GELU_SCALE = 0.7978845608028654
GELU_CUBIC = 0.044715
MESH = pl.DeviceIdType.MESH
VMEM_LIMIT = 48 * 1024 * 1024


def gelu_parts(preact):
    inner_arg = GELU_SCALE * (preact + GELU_CUBIC * preact * preact * preact)
    squash = jnp.tanh(inner_arg)
    gelu_value = 0.5 * preact * (1.0 + squash)
    derive = 0.5 * (1.0 + squash) + 0.5 * preact * (1.0 - squash * squash) * GELU_SCALE * (
        1.0 + 3.0 * GELU_CUBIC * preact * preact
    )
    return (gelu_value, derive)


def right_product(operand, weight):
    return lax.dot_general(
        operand, weight, (((1,), (1,)), ((), ())), preferred_element_type=jnp.float32
    )


class Grid:
    def __init__(self, n_dp, n_vocab):
        self.n_dp, self.n_vocab = n_dp, n_vocab
        self.cores = 2 if n_vocab % 2 == 0 else 1
        rest = n_vocab // self.cores
        self.outers = 4 if rest % 4 == 0 else 1
        self.mids = rest // self.outers

    def here(self):
        place = lax.axis_index("vocab")
        core = lax.rem(place, self.cores)
        chip = place // self.cores
        return lax.axis_index("dp"), chip // self.mids, lax.rem(chip, self.mids), core

    def index(self, outer, mid, core):
        return (outer * self.mids + mid) * self.cores + core

    def stepped(self, at, by, size):
        return lax.rem(at + by + size, size)

    def peers(self):
        dp, outer, mid, core = self.here()
        found = [(self.stepped(dp, s, self.n_dp), self.index(outer, mid, core)) for s in range(1, self.n_dp)]
        found += [(dp, self.index(self.stepped(outer, k, self.outers), mid, core)) for k in range(1, self.outers)]
        found += [(dp, self.index(outer, self.stepped(mid, j, self.mids), core)) for j in range(1, self.mids)]
        found += [(dp, self.index(outer, mid, self.stepped(core, c, self.cores))) for c in range(1, self.cores)]
        return found


def meet(peers):
    barrier = pltpu.get_barrier_semaphore()
    for peer in peers:
        pl.semaphore_signal(barrier, inc=1, device_id=peer, device_id_type=MESH)
    pl.semaphore_wait(barrier, len(peers))


def gather_kernel(grid, x_ref, out_ref, dp_send, dp_recv, send_sem, recv_sem, own_sem):
    dp, outer, mid, core = grid.here()
    me = grid.index(outer, mid, core)
    meet(grid.peers())
    sent = []

    def push(slot, target, count):
        copy = pltpu.make_async_remote_copy(
            src_ref=out_ref.at[slot], dst_ref=out_ref.at[slot], send_sem=send_sem.at[count],
            recv_sem=recv_sem.at[slot], device_id=target, device_id_type=MESH,
        )
        copy.start()
        sent.append(copy)

    def landed(slot):
        pltpu.make_async_remote_copy(
            src_ref=out_ref.at[slot], dst_ref=out_ref.at[slot], send_sem=send_sem.at[0],
            recv_sem=recv_sem.at[slot], device_id=(dp, me), device_id_type=MESH,
        ).wait_recv()

    first = []
    for s in range(1, grid.n_dp):
        other = grid.stepped(dp, s, grid.n_dp)
        copy = pltpu.make_async_remote_copy(
            src_ref=x_ref.at[other], dst_ref=out_ref.at[me, dp], send_sem=dp_send.at[s - 1],
            recv_sem=dp_recv.at[s - 1], device_id=(other, me), device_id_type=MESH,
        )
        copy.start()
        first.append(copy)
    own = pltpu.make_async_copy(x_ref.at[dp], out_ref.at[me, dp], own_sem)
    own.start()
    own.wait()
    for copy in first:
        copy.wait()

    count = 0
    for k in range(1, grid.outers):
        push(me, (dp, grid.index(grid.stepped(outer, k, grid.outers), mid, core)), count)
        count += 1
    for j in range(grid.mids):
        for k in range(grid.outers):
            slot = grid.index(grid.stepped(outer, -k, grid.outers), grid.stepped(mid, -j, grid.mids), core)
            if j or k:
                landed(slot)
            if j == 0:
                for i in range(1, grid.mids):
                    push(slot, (dp, grid.index(outer, grid.stepped(mid, i, grid.mids), core)), count)
                    count += 1
            for c in range(1, grid.cores):
                push(slot, (dp, grid.index(outer, mid, grid.stepped(core, c, grid.cores))), count)
                count += 1
    for c in range(1, grid.cores):
        for j in range(grid.mids):
            for k in range(grid.outers):
                landed(grid.index(
                    grid.stepped(outer, -k, grid.outers), grid.stepped(mid, -j, grid.mids),
                    grid.stepped(core, c, grid.cores),
                ))
    for copy in sent:
        copy.wait_send()


def vmem(count):
    return [pl.BlockSpec(memory_space=pltpu.VMEM)] * count


def gather_rows(grid, rows, ident):
    count, width = rows.shape
    part = width // grid.n_dp
    split = rows.reshape(count, grid.n_dp, part).transpose(1, 0, 2)
    sends = (grid.outers - 1) + grid.outers * (grid.mids - 1) + grid.outers * grid.mids * (grid.cores - 1)
    return pl.pallas_call(
        functools.partial(gather_kernel, grid),
        out_shape=jax.ShapeDtypeStruct((grid.n_vocab, grid.n_dp, count, part), rows.dtype),
        in_specs=vmem(1),
        out_specs=vmem(1)[0],
        scratch_shapes=[
            pltpu.SemaphoreType.DMA((max(grid.n_dp - 1, 1),)),
            pltpu.SemaphoreType.DMA((max(grid.n_dp - 1, 1),)),
            pltpu.SemaphoreType.DMA((max(sends, 1),)),
            pltpu.SemaphoreType.DMA((grid.n_vocab,)),
            pltpu.SemaphoreType.DMA,
        ],
        compiler_params=pltpu.CompilerParams(
            collective_id=ident, has_side_effects=True, vmem_limit_bytes=VMEM_LIMIT
        ),
        cost_estimate=pl.CostEstimate(flops=0, bytes_accessed=30_000_000, transcendentals=0),
        name="gather_rows",
    )(split)


def stats_kernel(grid, x_ref, out_ref, send_sem, recv_sem, own_sem):
    dp = lax.axis_index("dp")
    me = lax.axis_index("vocab")
    others = [lax.rem(me + k, grid.n_vocab) for k in range(1, grid.n_vocab)]
    meet([(dp, other) for other in others])
    copies = []
    for k, other in enumerate(others):
        copy = pltpu.make_async_remote_copy(
            src_ref=x_ref, dst_ref=out_ref.at[me], send_sem=send_sem.at[k],
            recv_sem=recv_sem.at[k], device_id=(dp, other), device_id_type=MESH,
        )
        copy.start()
        copies.append(copy)
    own = pltpu.make_async_copy(x_ref, out_ref.at[me], own_sem)
    own.start()
    own.wait()
    for copy in copies:
        copy.wait()


def gather_stats(grid, stats, ident):
    return pl.pallas_call(
        functools.partial(stats_kernel, grid),
        out_shape=jax.ShapeDtypeStruct((grid.n_vocab, *stats.shape), stats.dtype),
        in_specs=vmem(1),
        out_specs=vmem(1)[0],
        scratch_shapes=[
            pltpu.SemaphoreType.DMA((grid.n_vocab - 1,)),
            pltpu.SemaphoreType.DMA((grid.n_vocab - 1,)),
            pltpu.SemaphoreType.DMA,
        ],
        compiler_params=pltpu.CompilerParams(collective_id=ident, has_side_effects=True),
        cost_estimate=pl.CostEstimate(flops=0, bytes_accessed=15_000_000, transcendentals=0),
        name="gather_stats",
    )(stats)


def scatter_kernel(
    grid, count, x_ref, out_ref, core_in, mid_out, mid_in, outer_out, outer_in, last,
    core_send, core_recv, mid_send, mid_recv, outer_send, outer_recv, dp_send, dp_recv,
):
    dp, outer, mid, core = grid.here()
    me = grid.index(outer, mid, core)
    meet(grid.peers())
    outs, mids = grid.outers, grid.mids
    sent = []

    def push(src, dst, send, recv, target):
        copy = pltpu.make_async_remote_copy(
            src_ref=src, dst_ref=dst, send_sem=send, recv_sem=recv, device_id=target, device_id_type=MESH
        )
        copy.start()
        sent.append(copy)
        return copy

    order = [(j, k) for j in range(mids - 1, -1, -1) for k in range(outs - 1, -1, -1)]
    core_copies = {}
    for j, k in order:
        for c in range(1, grid.cores):
            away = grid.stepped(core, c, grid.cores)
            slot = grid.index(grid.stepped(outer, k, outs), grid.stepped(mid, j, mids), away)
            core_copies[j, k] = push(
                x_ref.at[slot], core_in.at[j, k], core_send.at[j, k], core_recv.at[j, k],
                (dp, grid.index(outer, mid, away)),
            )
    mid_copies = {}
    for j, k in order:
        own = x_ref[grid.index(grid.stepped(outer, k, outs), grid.stepped(mid, j, mids), core)]
        if grid.cores > 1:
            core_copies[j, k].wait_recv()
            own = own + core_in[j, k]
        if j:
            mid_out[j - 1, k] = own.astype(mid_out.dtype)
            mid_copies[j, k] = push(
                mid_out.at[j - 1, k], mid_in.at[j - 1, k], mid_send.at[j - 1, k], mid_recv.at[j - 1, k],
                (dp, grid.index(outer, grid.stepped(mid, j, mids), core)),
            )
        else:
            core_in[0, k] = own
    outer_copies = {}
    for k in range(outs - 1, -1, -1):
        total = core_in[0, k]
        for j in range(1, mids):
            mid_copies[j, k].wait_recv()
            total = total + mid_in[j - 1, k].astype(jnp.float32)
        if k:
            outer_out[k - 1] = total.astype(outer_out.dtype)
            outer_copies[k] = push(
                outer_out.at[k - 1], outer_in.at[k - 1], outer_send.at[k - 1], outer_recv.at[k - 1],
                (dp, grid.index(grid.stepped(outer, k, outs), mid, core)),
            )
        else:
            core_in[0, 0] = total
    total = core_in[0, 0]
    for k in range(1, outs):
        outer_copies[k].wait_recv()
        total = total + outer_in[k - 1].astype(jnp.float32)
    for n in range(grid.n_dp):
        last[n] = total[n * count:(n + 1) * count].astype(last.dtype)
    dp_copies = []
    for s in range(1, grid.n_dp):
        other = grid.stepped(dp, s, grid.n_dp)
        dp_copies.append(push(
            last.at[other], out_ref.at[dp], dp_send.at[s - 1], dp_recv.at[s - 1], (other, me)
        ))
    out_ref[dp] = last[dp]
    for copy in dp_copies:
        copy.wait_recv()
    for copy in sent:
        copy.wait_send()


def scatter_sum(grid, terms, count, ident):
    rows, part = terms.shape[1:]
    outs, mids = grid.outers, grid.mids
    dma = pltpu.SemaphoreType.DMA
    many, steps = max(mids - 1, 1), max(outs - 1, 1)
    result = pl.pallas_call(
        functools.partial(scatter_kernel, grid, count),
        out_shape=jax.ShapeDtypeStruct((grid.n_dp, count, part), jnp.bfloat16),
        in_specs=vmem(1),
        out_specs=vmem(1)[0],
        scratch_shapes=[
            pltpu.VMEM((mids, outs, rows, part), jnp.float32),
            pltpu.VMEM((many, outs, rows, part), jnp.bfloat16),
            pltpu.VMEM((many, outs, rows, part), jnp.bfloat16),
            pltpu.VMEM((steps, rows, part), jnp.bfloat16),
            pltpu.VMEM((steps, rows, part), jnp.bfloat16),
            pltpu.VMEM((grid.n_dp, count, part), jnp.bfloat16),
            dma((mids, outs)), dma((mids, outs)),
            dma((many, outs)), dma((many, outs)),
            dma((steps,)), dma((steps,)),
            dma((max(grid.n_dp - 1, 1),)), dma((max(grid.n_dp - 1, 1),)),
        ],
        compiler_params=pltpu.CompilerParams(
            collective_id=ident, has_side_effects=True, vmem_limit_bytes=VMEM_LIMIT
        ),
        cost_estimate=pl.CostEstimate(flops=0, bytes_accessed=60_000_000, transcendentals=0),
        name="scatter_sum",
    )(terms)
    return result.transpose(1, 0, 2).reshape(count, grid.n_dp * part)


def shifted(value, n_dp, step):
    return lax.ppermute(value, "dp", [(i, (i + step) % n_dp) for i in range(n_dp)])


def all_parts(value, n_dp):
    dp = lax.axis_index("dp")
    stacked = jnp.stack([value] + [shifted(value, n_dp, s) for s in range(1, n_dp)])
    return jnp.stack([
        lax.dynamic_index_in_dim(stacked, lax.rem(dp - n + n_dp, n_dp), 0, keepdims=False) for n in range(n_dp)
    ])


def summed(part, kind, n_dp):
    sent = part.astype(kind)
    total = part
    for s in range(1, n_dp):
        total = total + shifted(sent, n_dp, s).astype(jnp.float32)
    return total


def per_device(
    grid, hidden, targets, loss_weight, head_weight, gate_weight, up_weight, down_trans,
    block_input, block_cotangent,
):
    n_dp, n_vocab = grid.n_dp, grid.n_vocab
    rows, rows_b = hidden.shape[0], block_input.shape[0]
    part = head_weight.shape[0]

    def ordered(value):
        return all_parts(value, n_dp).reshape(n_dp, n_vocab, rows).transpose(1, 0, 2).reshape(-1)

    targets_all, weight_all = ordered(targets), ordered(loss_weight)

    head_rows = gather_rows(grid, hidden, 1).reshape(-1, part)
    logits_part = jnp.dot(head_rows, head_weight, preferred_element_type=jnp.float32)
    logits_sent = logits_part.astype(jnp.float16)
    both = jnp.concatenate([block_input, block_cotangent], axis=0)
    both, logits_sent = lax.optimization_barrier((both, logits_sent))
    logits = logits_part
    for s in range(1, n_dp):
        logits = logits + shifted(logits_sent, n_dp, s).astype(jnp.float32)

    both_all = gather_rows(grid, both, 2)
    in_rows = both_all[:, :, :rows_b].reshape(-1, part)
    cot_rows = both_all[:, :, rows_b:].reshape(-1, part)
    gate_pre = summed(jnp.dot(in_rows, gate_weight, preferred_element_type=jnp.float32), jnp.bfloat16, n_dp)
    up_pre = summed(jnp.dot(in_rows, up_weight, preferred_element_type=jnp.float32), jnp.bfloat16, n_dp)
    hidden_cot = summed(jnp.dot(cot_rows, down_trans, preferred_element_type=jnp.float32), jnp.bfloat16, n_dp)

    squash = jnp.tanh(logits / SOFTCAP)
    capped = SOFTCAP * squash
    cap_slope = 1.0 - squash * squash
    exponent = jnp.exp(capped)
    local_target = targets_all - lax.axis_index("vocab") * head_weight.shape[1]
    columns = lax.broadcasted_iota(jnp.int32, logits.shape, 1)
    target_mask = columns == local_target[:, None]
    part_total = jnp.sum(exponent, axis=1)
    part_target = jnp.sum(jnp.where(target_mask, capped, 0.0), axis=1)
    stats = jnp.stack([part_total, part_target]).reshape(-1, 128)
    stats_sum = jnp.sum(gather_stats(grid, stats, 3), axis=0).reshape(2, -1)
    exp_total, target_logit = stats_sum[0], stats_sum[1]
    onehot = jnp.where(target_mask, 1.0, 0.0)
    logit_cot = (
        weight_all[:, None] * (exponent / exp_total[:, None] - onehot) * cap_slope
    ).astype(jnp.bfloat16)
    head_terms = right_product(logit_cot, head_weight).reshape(n_vocab, n_dp * rows, part)
    loss_all = (jnp.log(exp_total) - target_logit).reshape(n_vocab, n_dp, rows)
    token_loss = lax.dynamic_index_in_dim(loss_all, lax.axis_index("dp"), 1, keepdims=False).reshape(-1)
    head_out = scatter_sum(grid, head_terms, rows, 4)

    gate_act, derive = gelu_parts(gate_pre)
    gate_cot = (hidden_cot * up_pre * derive).astype(jnp.bfloat16)
    up_cot = (hidden_cot * gate_act).astype(jnp.bfloat16)
    block_terms = right_product(gate_cot, gate_weight) + right_product(up_cot, up_weight)
    block_out = scatter_sum(grid, block_terms.reshape(n_vocab, n_dp * rows_b, part), rows_b, 5)
    return (token_loss, head_out, block_out)


def solution(mesh):
    grid = Grid(mesh.shape["dp"], mesh.shape["vocab"])
    return jax.shard_map(
        functools.partial(per_device, grid),
        mesh=mesh,
        in_specs=(
            P(("dp", "vocab"), None),
            P("dp"),
            P("dp"),
            P("dp", "vocab"),
            P("dp", "vocab"),
            P("dp", "vocab"),
            P("dp", "vocab"),
            P(("dp", "vocab"), None),
            P(("dp", "vocab"), None),
        ),
        out_specs=(P("dp"), P(("dp", "vocab"), None), P(("dp", "vocab"), None)),
        check_vma=False,
    )
```

```python
import functools

import jax
import jax.numpy as jnp
from jax import lax
from jax.experimental import pallas as pl
from jax.experimental.pallas import tpu as pltpu
from jax.sharding import PartitionSpec as P

SOFTCAP = 30.0
GELU_SCALE = 0.7978845608028654
GELU_CUBIC = 0.044715
MESH = pl.DeviceIdType.MESH
VMEM_LIMIT = 48 * 1024 * 1024


def gelu_parts(preact):
    inner_arg = GELU_SCALE * (preact + GELU_CUBIC * preact * preact * preact)
    squash = jnp.tanh(inner_arg)
    gelu_value = 0.5 * preact * (1.0 + squash)
    derive = 0.5 * (1.0 + squash) + 0.5 * preact * (1.0 - squash * squash) * GELU_SCALE * (
        1.0 + 3.0 * GELU_CUBIC * preact * preact
    )
    return (gelu_value, derive)


def right_product(operand, weight):
    return lax.dot_general(
        operand, weight, (((1,), (1,)), ((), ())), preferred_element_type=jnp.float32
    )


class Grid:
    def __init__(self, n_dp, n_vocab):
        self.n_dp, self.n_vocab = n_dp, n_vocab
        self.cores = 2 if n_vocab % 2 == 0 else 1
        rest = n_vocab // self.cores
        self.outers = 4 if rest % 4 == 0 else 1
        self.mids = rest // self.outers

    def here(self):
        place = lax.axis_index("vocab")
        core = lax.rem(place, self.cores)
        chip = place // self.cores
        return lax.axis_index("dp"), chip // self.mids, lax.rem(chip, self.mids), core

    def index(self, outer, mid, core):
        return (outer * self.mids + mid) * self.cores + core

    def stepped(self, at, by, size):
        return lax.rem(at + by + size, size)

    def peers(self):
        dp, outer, mid, core = self.here()
        found = [(self.stepped(dp, s, self.n_dp), self.index(outer, mid, core)) for s in range(1, self.n_dp)]
        found += [(dp, self.index(self.stepped(outer, k, self.outers), mid, core)) for k in range(1, self.outers)]
        found += [(dp, self.index(outer, self.stepped(mid, j, self.mids), core)) for j in range(1, self.mids)]
        found += [(dp, self.index(outer, mid, self.stepped(core, c, self.cores))) for c in range(1, self.cores)]
        return found


def meet(peers):
    barrier = pltpu.get_barrier_semaphore()
    for peer in peers:
        pl.semaphore_signal(barrier, inc=1, device_id=peer, device_id_type=MESH)
    pl.semaphore_wait(barrier, len(peers))


def gather_kernel(grid, has_dp, *refs):
    if has_dp:
        x_ref, late_ref, out_ref, late_out, dp_send, dp_recv, late_send, late_recv, send_sem, recv_sem, own_sem = refs
    else:
        x_ref, out_ref, send_sem, recv_sem, own_sem = refs
    dp, outer, mid, core = grid.here()
    me = grid.index(outer, mid, core)
    everyone = grid.peers()
    meet(everyone if has_dp else everyone[grid.n_dp - 1:])
    sent = []

    def push(slot, part, target, step):
        copy = pltpu.make_async_remote_copy(
            src_ref=out_ref.at[slot, part], dst_ref=out_ref.at[slot, part], send_sem=send_sem.at[len(sent)],
            recv_sem=recv_sem.at[slot, step], device_id=target, device_id_type=MESH,
        )
        copy.start()
        sent.append(copy)

    def landed(slot, part, step):
        pltpu.make_async_remote_copy(
            src_ref=out_ref.at[slot, part], dst_ref=out_ref.at[slot, part], send_sem=send_sem.at[0],
            recv_sem=recv_sem.at[slot, step], device_id=(dp, me), device_id_type=MESH,
        ).wait_recv()

    first, late = [], []
    if has_dp:
        for s in range(1, grid.n_dp):
            other = grid.stepped(dp, s, grid.n_dp)
            for group, src, dst, send, recv in (
                (first, x_ref.at[other], out_ref.at[me, dp], dp_send, dp_recv),
                (late, late_ref.at[other], late_out.at[dp], late_send, late_recv),
            ):
                copy = pltpu.make_async_remote_copy(
                    src_ref=src, dst_ref=dst, send_sem=send.at[s - 1], recv_sem=recv.at[s - 1],
                    device_id=(other, me), device_id_type=MESH,
                )
                copy.start()
                group.append(copy)
        owns = [
            pltpu.make_async_copy(x_ref.at[dp], out_ref.at[me, dp], own_sem.at[0]),
            pltpu.make_async_copy(late_ref.at[dp], late_out.at[dp], own_sem.at[1]),
        ]
    else:
        owns = [pltpu.make_async_copy(x_ref, out_ref.at[me], own_sem.at[0])]
    for own in owns:
        own.start()
    for own in owns:
        own.wait()

    def beside(slot, part, step):
        for c in range(1, grid.cores):
            push(slot, part, (dp, grid.index(outer, mid, grid.stepped(core, c, grid.cores))), step)

    def across(slot, part, step):
        for i in range(1, grid.mids):
            push(slot, part, (dp, grid.index(outer, grid.stepped(mid, i, grid.mids), core)), step)

    for step in range(grid.n_dp):
        part = grid.stepped(dp, -step, grid.n_dp)
        if has_dp and step:
            first[step - 1].wait_recv()
        for k in range(grid.outers - 1, 0, -1):
            push(me, part, (dp, grid.index(grid.stepped(outer, k, grid.outers), mid, core)), step)
        across(me, part, step)
        beside(me, part, step)
    for step in range(grid.n_dp):
        part = grid.stepped(dp, -step, grid.n_dp)
        for k in range(1, grid.outers):
            slot = grid.index(grid.stepped(outer, -k, grid.outers), mid, core)
            landed(slot, part, step)
            across(slot, part, step)
            beside(slot, part, step)
    for step in range(grid.n_dp):
        part = grid.stepped(dp, -step, grid.n_dp)
        for j in range(1, grid.mids):
            for k in range(grid.outers):
                slot = grid.index(grid.stepped(outer, -k, grid.outers), grid.stepped(mid, -j, grid.mids), core)
                landed(slot, part, step)
                beside(slot, part, step)
    for c in range(1, grid.cores):
        for step in range(grid.n_dp):
            part = grid.stepped(dp, -step, grid.n_dp)
            for j in range(grid.mids):
                for k in range(grid.outers):
                    landed(grid.index(
                        grid.stepped(outer, -k, grid.outers), grid.stepped(mid, -j, grid.mids),
                        grid.stepped(core, c, grid.cores),
                    ), part, step)
    for copy in late:
        copy.wait_recv()
    for copy in sent + first + late:
        copy.wait_send()


def vmem(count):
    return [pl.BlockSpec(memory_space=pltpu.VMEM)] * count


def split_features(grid, rows):
    count, width = rows.shape
    return rows.reshape(count, grid.n_dp, width // grid.n_dp).transpose(1, 0, 2)


def gather_rows(grid, rows, late, ident):
    has_dp = late is not None
    n_dp, count, part = rows.shape
    sends = (grid.outers - 1) + grid.outers * (grid.mids - 1) + grid.outers * grid.mids * (grid.cores - 1)
    dma = pltpu.SemaphoreType.DMA
    pair = (max(n_dp - 1, 1),)
    out = jax.ShapeDtypeStruct((grid.n_vocab, n_dp, count, part), rows.dtype)
    moved = [rows] + ([late] if has_dp else [])
    shapes = [out] + ([jax.ShapeDtypeStruct(late.shape, late.dtype)] if has_dp else [])
    return pl.pallas_call(
        functools.partial(gather_kernel, grid, has_dp),
        out_shape=shapes,
        in_specs=vmem(len(moved)),
        out_specs=vmem(len(shapes)),
        scratch_shapes=([dma(pair)] * 4 if has_dp else [])
        + [dma((max(sends, 1) * n_dp,)), dma((grid.n_vocab, n_dp)), dma((2,))],
        compiler_params=pltpu.CompilerParams(
            collective_id=ident, has_side_effects=True, vmem_limit_bytes=VMEM_LIMIT
        ),
        cost_estimate=pl.CostEstimate(flops=0, bytes_accessed=30_000_000, transcendentals=0),
        name="gather_rows",
    )(*moved)


def stats_kernel(grid, x_ref, out_ref, send_sem, recv_sem, own_sem):
    dp = lax.axis_index("dp")
    me = lax.axis_index("vocab")
    others = [lax.rem(me + k, grid.n_vocab) for k in range(1, grid.n_vocab)]
    meet([(dp, other) for other in others])
    copies = []
    for k, other in enumerate(others):
        copy = pltpu.make_async_remote_copy(
            src_ref=x_ref, dst_ref=out_ref.at[me], send_sem=send_sem.at[k],
            recv_sem=recv_sem.at[k], device_id=(dp, other), device_id_type=MESH,
        )
        copy.start()
        copies.append(copy)
    own = pltpu.make_async_copy(x_ref, out_ref.at[me], own_sem)
    own.start()
    own.wait()
    for copy in copies:
        copy.wait()


def gather_stats(grid, stats, ident):
    return pl.pallas_call(
        functools.partial(stats_kernel, grid),
        out_shape=jax.ShapeDtypeStruct((grid.n_vocab, *stats.shape), stats.dtype),
        in_specs=vmem(1),
        out_specs=vmem(1)[0],
        scratch_shapes=[
            pltpu.SemaphoreType.DMA((grid.n_vocab - 1,)),
            pltpu.SemaphoreType.DMA((grid.n_vocab - 1,)),
            pltpu.SemaphoreType.DMA,
        ],
        compiler_params=pltpu.CompilerParams(collective_id=ident, has_side_effects=True),
        cost_estimate=pl.CostEstimate(flops=0, bytes_accessed=15_000_000, transcendentals=0),
        name="gather_stats",
    )(stats)


def scatter_kernel(
    grid, count, x_ref, out_ref, core_in, mid_out, mid_in, outer_out, outer_in, last,
    core_send, core_recv, mid_send, mid_recv, outer_send, outer_recv, dp_send, dp_recv,
):
    dp, outer, mid, core = grid.here()
    me = grid.index(outer, mid, core)
    meet(grid.peers())
    outs, mids = grid.outers, grid.mids
    sent = []

    def push(src, dst, send, recv, target):
        copy = pltpu.make_async_remote_copy(
            src_ref=src, dst_ref=dst, send_sem=send, recv_sem=recv, device_id=target, device_id_type=MESH
        )
        copy.start()
        sent.append(copy)
        return copy

    order = [(j, k) for j in range(mids - 1, -1, -1) for k in range(outs - 1, -1, -1)]
    core_copies = {}
    for j, k in order:
        for c in range(1, grid.cores):
            away = grid.stepped(core, c, grid.cores)
            slot = grid.index(grid.stepped(outer, k, outs), grid.stepped(mid, j, mids), away)
            core_copies[j, k] = push(
                x_ref.at[slot], core_in.at[j, k], core_send.at[j, k], core_recv.at[j, k],
                (dp, grid.index(outer, mid, away)),
            )
    mid_copies = {}
    for j, k in order:
        own = x_ref[grid.index(grid.stepped(outer, k, outs), grid.stepped(mid, j, mids), core)]
        if grid.cores > 1:
            core_copies[j, k].wait_recv()
            own = own + core_in[j, k]
        if j:
            mid_out[j - 1, k] = own.astype(mid_out.dtype)
            mid_copies[j, k] = push(
                mid_out.at[j - 1, k], mid_in.at[j - 1, k], mid_send.at[j - 1, k], mid_recv.at[j - 1, k],
                (dp, grid.index(outer, grid.stepped(mid, j, mids), core)),
            )
        else:
            core_in[0, k] = own
    outer_copies = {}
    for k in range(outs - 1, -1, -1):
        total = core_in[0, k]
        for j in range(1, mids):
            mid_copies[j, k].wait_recv()
            total = total + mid_in[j - 1, k].astype(jnp.float32)
        if k:
            outer_out[k - 1] = total.astype(outer_out.dtype)
            outer_copies[k] = push(
                outer_out.at[k - 1], outer_in.at[k - 1], outer_send.at[k - 1], outer_recv.at[k - 1],
                (dp, grid.index(grid.stepped(outer, k, outs), mid, core)),
            )
        else:
            core_in[0, 0] = total
    total = core_in[0, 0]
    for k in range(1, outs):
        outer_copies[k].wait_recv()
        total = total + outer_in[k - 1].astype(jnp.float32)
    for n in range(grid.n_dp):
        last[n] = total[n * count:(n + 1) * count].astype(last.dtype)
    dp_copies = []
    for s in range(1, grid.n_dp):
        other = grid.stepped(dp, s, grid.n_dp)
        dp_copies.append(push(
            last.at[other], out_ref.at[dp], dp_send.at[s - 1], dp_recv.at[s - 1], (other, me)
        ))
    out_ref[dp] = last[dp]
    for copy in dp_copies:
        copy.wait_recv()
    for copy in sent:
        copy.wait_send()


def scatter_sum(grid, terms, count, ident):
    rows, part = terms.shape[1:]
    outs, mids = grid.outers, grid.mids
    dma = pltpu.SemaphoreType.DMA
    many, steps = max(mids - 1, 1), max(outs - 1, 1)
    result = pl.pallas_call(
        functools.partial(scatter_kernel, grid, count),
        out_shape=jax.ShapeDtypeStruct((grid.n_dp, count, part), jnp.bfloat16),
        in_specs=vmem(1),
        out_specs=vmem(1)[0],
        scratch_shapes=[
            pltpu.VMEM((mids, outs, rows, part), jnp.float32),
            pltpu.VMEM((many, outs, rows, part), jnp.bfloat16),
            pltpu.VMEM((many, outs, rows, part), jnp.bfloat16),
            pltpu.VMEM((steps, rows, part), jnp.bfloat16),
            pltpu.VMEM((steps, rows, part), jnp.bfloat16),
            pltpu.VMEM((grid.n_dp, count, part), jnp.bfloat16),
            dma((mids, outs)), dma((mids, outs)),
            dma((many, outs)), dma((many, outs)),
            dma((steps,)), dma((steps,)),
            dma((max(grid.n_dp - 1, 1),)), dma((max(grid.n_dp - 1, 1),)),
        ],
        compiler_params=pltpu.CompilerParams(
            collective_id=ident, has_side_effects=True, vmem_limit_bytes=VMEM_LIMIT
        ),
        cost_estimate=pl.CostEstimate(flops=0, bytes_accessed=60_000_000, transcendentals=0),
        name="scatter_sum",
    )(terms)
    return result.transpose(1, 0, 2).reshape(count, grid.n_dp * part)


def shifted(value, n_dp, step):
    return lax.ppermute(value, "dp", [(i, (i + step) % n_dp) for i in range(n_dp)])


def all_parts(value, n_dp):
    dp = lax.axis_index("dp")
    stacked = jnp.stack([value] + [shifted(value, n_dp, s) for s in range(1, n_dp)])
    return jnp.stack([
        lax.dynamic_index_in_dim(stacked, lax.rem(dp - n + n_dp, n_dp), 0, keepdims=False) for n in range(n_dp)
    ])


def exchanged(part, kind, n_dp):
    sent = part.astype(kind)
    return [shifted(sent, n_dp, s) for s in range(1, n_dp)]


def total_of(part, others):
    for other in others:
        part = part + other.astype(jnp.float32)
    return part


CHUNKS = 2


def per_device(
    grid, hidden, targets, loss_weight, head_weight, gate_weight, up_weight, down_trans,
    block_input, block_cotangent,
):
    n_dp, n_vocab = grid.n_dp, grid.n_vocab
    rows, rows_b = hidden.shape[0], block_input.shape[0]
    part = head_weight.shape[0]

    def ordered(value):
        return all_parts(value, n_dp).reshape(n_dp, n_vocab, rows).transpose(1, 0, 2).reshape(-1)

    both = jnp.concatenate([block_input, block_cotangent], axis=0)
    head_rows, both_part = gather_rows(grid, split_features(grid, hidden), split_features(grid, both), 1)
    targets_all, weight_all = ordered(targets), ordered(loss_weight)
    local_target = targets_all - lax.axis_index("vocab") * head_weight.shape[1]

    chunk = n_vocab // CHUNKS
    parts, others = [], []
    for c in range(CHUNKS):
        chunk_rows = head_rows[c * chunk:(c + 1) * chunk].reshape(-1, part)
        if c:
            chunk_rows, _ = lax.optimization_barrier((chunk_rows, parts[-1]))
        product = jnp.dot(chunk_rows, head_weight, preferred_element_type=jnp.float32)
        sent = product.astype(jnp.float16)
        parts.append(product)
        others.append([shifted(sent, n_dp, s) for s in range(1, n_dp)])
    both_part, _ = lax.optimization_barrier((both_part, parts[-1]))

    both_all, = gather_rows(grid, both_part, None, 2)
    in_rows = both_all[:, :, :rows_b].reshape(-1, part)
    cot_rows = both_all[:, :, rows_b:].reshape(-1, part)
    gate_part = jnp.dot(in_rows, gate_weight, preferred_element_type=jnp.float32)
    up_part = jnp.dot(in_rows, up_weight, preferred_element_type=jnp.float32)
    cot_part = jnp.dot(cot_rows, down_trans, preferred_element_type=jnp.float32)
    gate_others = exchanged(gate_part, jnp.bfloat16, n_dp)
    up_others = exchanged(up_part, jnp.bfloat16, n_dp)
    cot_others = exchanged(cot_part, jnp.bfloat16, n_dp)

    scaled, masks, totals, hits, slopes = [], [], [], [], []
    for c in range(CHUNKS):
        logits = total_of(parts[c], others[c])
        squash = jnp.tanh(logits / SOFTCAP)
        capped = SOFTCAP * squash
        cap_slope = 1.0 - squash * squash
        exponent = jnp.exp(capped)
        columns = lax.broadcasted_iota(jnp.int32, logits.shape, 1)
        size = logits.shape[0]
        mask = columns == local_target[c * size:(c + 1) * size, None]
        scaled.append(exponent * cap_slope)
        masks.append(mask)
        totals.append(jnp.sum(exponent, axis=1))
        hits.append(jnp.sum(jnp.where(mask, capped, 0.0), axis=1))
        slopes.append(jnp.sum(jnp.where(mask, cap_slope, 0.0), axis=1))
    scaled, totals, hits, slopes = lax.optimization_barrier((scaled, totals, hits, slopes))
    stats = jnp.concatenate(totals + hits).reshape(-1, 128)
    stats_sum = jnp.sum(gather_stats(grid, stats, 3), axis=0).reshape(2, -1)
    exp_total, target_logit = stats_sum[0], stats_sum[1]
    share = weight_all / exp_total
    target_share = weight_all * jnp.concatenate(slopes)
    head_terms = []
    for c in range(CHUNKS):
        size = scaled[c].shape[0]
        span = slice(c * size, (c + 1) * size)
        logit_cot = (
            share[span, None] * scaled[c] - jnp.where(masks[c], target_share[span, None], 0.0)
        ).astype(jnp.bfloat16)
        head_terms.append(right_product(logit_cot, head_weight).reshape(chunk, n_dp * rows, part))
    loss_all = (jnp.log(exp_total) - target_logit).reshape(n_vocab, n_dp, rows)
    token_loss = lax.dynamic_index_in_dim(loss_all, lax.axis_index("dp"), 1, keepdims=False).reshape(-1)
    head_out = scatter_sum(grid, jnp.concatenate(head_terms, axis=0), rows, 4)

    gate_others, up_others, cot_others, head_out = lax.optimization_barrier(
        (gate_others, up_others, cot_others, head_out)
    )
    gate_pre = total_of(gate_part, gate_others)
    up_pre = total_of(up_part, up_others)
    hidden_cot = total_of(cot_part, cot_others)
    gate_act, derive = gelu_parts(gate_pre)
    gate_cot = (hidden_cot * up_pre * derive).astype(jnp.bfloat16)
    up_cot = (hidden_cot * gate_act).astype(jnp.bfloat16)
    block_terms = right_product(gate_cot, gate_weight) + right_product(up_cot, up_weight)
    block_out = scatter_sum(grid, block_terms.reshape(n_vocab, n_dp * rows_b, part), rows_b, 5)
    return (token_loss, head_out, block_out)


def solution(mesh):
    grid = Grid(mesh.shape["dp"], mesh.shape["vocab"])
    return jax.shard_map(
        functools.partial(per_device, grid),
        mesh=mesh,
        in_specs=(
            P(("dp", "vocab"), None),
            P("dp"),
            P("dp"),
            P("dp", "vocab"),
            P("dp", "vocab"),
            P("dp", "vocab"),
            P("dp", "vocab"),
            P(("dp", "vocab"), None),
            P(("dp", "vocab"), None),
        ),
        out_specs=(P("dp"), P(("dp", "vocab"), None), P(("dp", "vocab"), None)),
        check_vma=False,
    )
```

```python
import functools

import jax
import jax.numpy as jnp
from jax import lax
from jax.experimental import pallas as pl
from jax.experimental.pallas import tpu as pltpu
from jax.sharding import PartitionSpec as P

SOFTCAP = 30.0
GELU_SCALE = 0.7978845608028654
GELU_CUBIC = 0.044715
MESH = pl.DeviceIdType.MESH
VMEM_LIMIT = 48 * 1024 * 1024


def gelu_parts(preact):
    inner_arg = GELU_SCALE * (preact + GELU_CUBIC * preact * preact * preact)
    squash = jnp.tanh(inner_arg)
    gelu_value = 0.5 * preact * (1.0 + squash)
    derive = 0.5 * (1.0 + squash) + 0.5 * preact * (1.0 - squash * squash) * GELU_SCALE * (
        1.0 + 3.0 * GELU_CUBIC * preact * preact
    )
    return (gelu_value, derive)


def right_product(operand, weight):
    return lax.dot_general(
        operand, weight, (((1,), (1,)), ((), ())), preferred_element_type=jnp.float32
    )


class Grid:
    def __init__(self, n_dp, n_vocab):
        self.n_dp, self.n_vocab = n_dp, n_vocab
        self.cores = 2 if n_vocab % 2 == 0 else 1
        rest = n_vocab // self.cores
        self.outers = 4 if rest % 4 == 0 else 1
        self.mids = rest // self.outers

    def here(self):
        place = lax.axis_index("vocab")
        core = lax.rem(place, self.cores)
        chip = place // self.cores
        return lax.axis_index("dp"), chip // self.mids, lax.rem(chip, self.mids), core

    def index(self, outer, mid, core):
        return (outer * self.mids + mid) * self.cores + core

    def stepped(self, at, by, size):
        return lax.rem(at + by + size, size)

    def peers(self):
        dp, outer, mid, core = self.here()
        found = [(self.stepped(dp, s, self.n_dp), self.index(outer, mid, core)) for s in range(1, self.n_dp)]
        found += [(dp, self.index(self.stepped(outer, k, self.outers), mid, core)) for k in range(1, self.outers)]
        found += [(dp, self.index(outer, self.stepped(mid, j, self.mids), core)) for j in range(1, self.mids)]
        found += [(dp, self.index(outer, mid, self.stepped(core, c, self.cores))) for c in range(1, self.cores)]
        return found


def meet(peers):
    barrier = pltpu.get_barrier_semaphore()
    for peer in peers:
        pl.semaphore_signal(barrier, inc=1, device_id=peer, device_id_type=MESH)
    pl.semaphore_wait(barrier, len(peers))


def gather_kernel(grid, has_dp, *refs):
    if has_dp:
        x_ref, late_ref, out_ref, late_out, dp_send, dp_recv, late_send, late_recv, send_sem, recv_sem, own_sem = refs
    else:
        x_ref, out_ref, send_sem, recv_sem, own_sem = refs
    dp, outer, mid, core = grid.here()
    me = grid.index(outer, mid, core)
    everyone = grid.peers()
    meet(everyone if has_dp else everyone[grid.n_dp - 1:])
    sent = []

    def push(slot, part, target, step):
        copy = pltpu.make_async_remote_copy(
            src_ref=out_ref.at[slot, part], dst_ref=out_ref.at[slot, part], send_sem=send_sem.at[len(sent)],
            recv_sem=recv_sem.at[slot, step], device_id=target, device_id_type=MESH,
        )
        copy.start()
        sent.append(copy)

    def landed(slot, part, step):
        pltpu.make_async_remote_copy(
            src_ref=out_ref.at[slot, part], dst_ref=out_ref.at[slot, part], send_sem=send_sem.at[0],
            recv_sem=recv_sem.at[slot, step], device_id=(dp, me), device_id_type=MESH,
        ).wait_recv()

    first, late = [], []
    if has_dp:
        for s in range(1, grid.n_dp):
            other = grid.stepped(dp, s, grid.n_dp)
            for group, src, dst, send, recv in (
                (first, x_ref.at[other], out_ref.at[me, dp], dp_send, dp_recv),
                (late, late_ref.at[other], late_out.at[dp], late_send, late_recv),
            ):
                copy = pltpu.make_async_remote_copy(
                    src_ref=src, dst_ref=dst, send_sem=send.at[s - 1], recv_sem=recv.at[s - 1],
                    device_id=(other, me), device_id_type=MESH,
                )
                copy.start()
                group.append(copy)
        owns = [
            pltpu.make_async_copy(x_ref.at[dp], out_ref.at[me, dp], own_sem.at[0]),
            pltpu.make_async_copy(late_ref.at[dp], late_out.at[dp], own_sem.at[1]),
        ]
    else:
        owns = [pltpu.make_async_copy(x_ref, out_ref.at[me], own_sem.at[0])]
    for own in owns:
        own.start()
    for own in owns:
        own.wait()

    def beside(slot, part, step):
        for c in range(1, grid.cores):
            push(slot, part, (dp, grid.index(outer, mid, grid.stepped(core, c, grid.cores))), step)

    def across(slot, part, step):
        for i in range(1, grid.mids):
            push(slot, part, (dp, grid.index(outer, grid.stepped(mid, i, grid.mids), core)), step)

    for step in range(grid.n_dp):
        part = grid.stepped(dp, -step, grid.n_dp)
        if has_dp and step:
            first[step - 1].wait_recv()
        for k in range(grid.outers - 1, 0, -1):
            push(me, part, (dp, grid.index(grid.stepped(outer, k, grid.outers), mid, core)), step)
        across(me, part, step)
        beside(me, part, step)
    for step in range(grid.n_dp):
        part = grid.stepped(dp, -step, grid.n_dp)
        for k in range(1, grid.outers):
            slot = grid.index(grid.stepped(outer, -k, grid.outers), mid, core)
            landed(slot, part, step)
            across(slot, part, step)
            beside(slot, part, step)
    for step in range(grid.n_dp):
        part = grid.stepped(dp, -step, grid.n_dp)
        for j in range(1, grid.mids):
            for k in range(grid.outers):
                slot = grid.index(grid.stepped(outer, -k, grid.outers), grid.stepped(mid, -j, grid.mids), core)
                landed(slot, part, step)
                beside(slot, part, step)
    for c in range(1, grid.cores):
        for step in range(grid.n_dp):
            part = grid.stepped(dp, -step, grid.n_dp)
            for j in range(grid.mids):
                for k in range(grid.outers):
                    landed(grid.index(
                        grid.stepped(outer, -k, grid.outers), grid.stepped(mid, -j, grid.mids),
                        grid.stepped(core, c, grid.cores),
                    ), part, step)
    for copy in late:
        copy.wait_recv()
    for copy in sent + first + late:
        copy.wait_send()


def vmem(count):
    return [pl.BlockSpec(memory_space=pltpu.VMEM)] * count


def split_features(grid, rows):
    count, width = rows.shape
    return rows.reshape(count, grid.n_dp, width // grid.n_dp).transpose(1, 0, 2)


def gather_rows(grid, rows, late, ident):
    has_dp = late is not None
    n_dp, count, part = rows.shape
    sends = (grid.outers - 1) + grid.outers * (grid.mids - 1) + grid.outers * grid.mids * (grid.cores - 1)
    dma = pltpu.SemaphoreType.DMA
    pair = (max(n_dp - 1, 1),)
    out = jax.ShapeDtypeStruct((grid.n_vocab, n_dp, count, part), rows.dtype)
    moved = [rows] + ([late] if has_dp else [])
    shapes = [out] + ([jax.ShapeDtypeStruct(late.shape, late.dtype)] if has_dp else [])
    return pl.pallas_call(
        functools.partial(gather_kernel, grid, has_dp),
        out_shape=shapes,
        in_specs=vmem(len(moved)),
        out_specs=vmem(len(shapes)),
        scratch_shapes=([dma(pair)] * 4 if has_dp else [])
        + [dma((max(sends, 1) * n_dp,)), dma((grid.n_vocab, n_dp)), dma((2,))],
        compiler_params=pltpu.CompilerParams(
            collective_id=ident, has_side_effects=True, vmem_limit_bytes=VMEM_LIMIT
        ),
        cost_estimate=pl.CostEstimate(flops=0, bytes_accessed=30_000_000, transcendentals=0),
        name="gather_rows",
    )(*moved)


def stats_kernel(grid, x_ref, out_ref, send_sem, recv_sem, own_sem):
    dp = lax.axis_index("dp")
    me = lax.axis_index("vocab")
    others = [lax.rem(me + k, grid.n_vocab) for k in range(1, grid.n_vocab)]
    meet([(dp, other) for other in others])
    copies = []
    for k, other in enumerate(others):
        copy = pltpu.make_async_remote_copy(
            src_ref=x_ref, dst_ref=out_ref.at[me], send_sem=send_sem.at[k],
            recv_sem=recv_sem.at[k], device_id=(dp, other), device_id_type=MESH,
        )
        copy.start()
        copies.append(copy)
    own = pltpu.make_async_copy(x_ref, out_ref.at[me], own_sem)
    own.start()
    own.wait()
    for copy in copies:
        copy.wait()


def gather_stats(grid, stats, ident):
    return pl.pallas_call(
        functools.partial(stats_kernel, grid),
        out_shape=jax.ShapeDtypeStruct((grid.n_vocab, *stats.shape), stats.dtype),
        in_specs=vmem(1),
        out_specs=vmem(1)[0],
        scratch_shapes=[
            pltpu.SemaphoreType.DMA((grid.n_vocab - 1,)),
            pltpu.SemaphoreType.DMA((grid.n_vocab - 1,)),
            pltpu.SemaphoreType.DMA,
        ],
        compiler_params=pltpu.CompilerParams(collective_id=ident, has_side_effects=True),
        cost_estimate=pl.CostEstimate(flops=0, bytes_accessed=15_000_000, transcendentals=0),
        name="gather_stats",
    )(stats)


def scatter_kernel(grid, counts, *refs):
    many = len(counts)
    x_refs, out_refs, scratch = refs[:many], refs[many:2 * many], refs[2 * many:]
    held = [scratch[14 * p:14 * p + 14] for p in range(many)]
    dp, outer, mid, core = grid.here()
    me = grid.index(outer, mid, core)
    meet(grid.peers())
    outs, mids = grid.outers, grid.mids
    sent = []

    def push(src, dst, send, recv, target):
        copy = pltpu.make_async_remote_copy(
            src_ref=src, dst_ref=dst, send_sem=send, recv_sem=recv, device_id=target, device_id_type=MESH
        )
        copy.start()
        sent.append(copy)
        return copy

    order = [(p, j, k) for p in range(many) for j in range(mids - 1, -1, -1) for k in range(outs - 1, -1, -1)]
    order.sort(key=lambda step: -step[1])
    core_copies, mid_copies, outer_copies, dp_copies = {}, {}, {}, []
    for p, j, k in order:
        core_in, send, recv = held[p][0], held[p][6], held[p][7]
        for c in range(1, grid.cores):
            away = grid.stepped(core, c, grid.cores)
            slot = grid.index(grid.stepped(outer, k, outs), grid.stepped(mid, j, mids), away)
            core_copies[p, j, k] = push(
                x_refs[p].at[slot], core_in.at[j, k], send.at[j, k], recv.at[j, k],
                (dp, grid.index(outer, mid, away)),
            )
    for p, j, k in order:
        core_in, mid_out, mid_in, send, recv = held[p][0], held[p][1], held[p][2], held[p][8], held[p][9]
        own = x_refs[p][grid.index(grid.stepped(outer, k, outs), grid.stepped(mid, j, mids), core)]
        if grid.cores > 1:
            core_copies[p, j, k].wait_recv()
            own = own + core_in[j, k]
        if j:
            mid_out[j - 1, k] = own.astype(mid_out.dtype)
            mid_copies[p, j, k] = push(
                mid_out.at[j - 1, k], mid_in.at[j - 1, k], send.at[j - 1, k], recv.at[j - 1, k],
                (dp, grid.index(outer, grid.stepped(mid, j, mids), core)),
            )
        else:
            core_in[0, k] = own
    for p in range(many):
        core_in, mid_in, outer_out, outer_in, send, recv = held[p][0], *held[p][2:5], held[p][10], held[p][11]
        for k in range(outs - 1, -1, -1):
            total = core_in[0, k]
            for j in range(1, mids):
                mid_copies[p, j, k].wait_recv()
                total = total + mid_in[j - 1, k].astype(jnp.float32)
            if k:
                outer_out[k - 1] = total.astype(outer_out.dtype)
                outer_copies[p, k] = push(
                    outer_out.at[k - 1], outer_in.at[k - 1], send.at[k - 1], recv.at[k - 1],
                    (dp, grid.index(grid.stepped(outer, k, outs), mid, core)),
                )
            else:
                core_in[0, 0] = total
    for p in range(many):
        core_in, outer_in, last, send, recv = held[p][0], held[p][4], held[p][5], held[p][12], held[p][13]
        count = counts[p]
        total = core_in[0, 0]
        for k in range(1, outs):
            outer_copies[p, k].wait_recv()
            total = total + outer_in[k - 1].astype(jnp.float32)
        for n in range(grid.n_dp):
            last[n] = total[n * count:(n + 1) * count].astype(last.dtype)
        for s in range(1, grid.n_dp):
            other = grid.stepped(dp, s, grid.n_dp)
            dp_copies.append(push(
                last.at[other], out_refs[p].at[dp], send.at[s - 1], recv.at[s - 1], (other, me)
            ))
        out_refs[p][dp] = last[dp]
    for copy in dp_copies:
        copy.wait_recv()
    for copy in sent:
        copy.wait_send()


def scatter_sums(grid, terms, counts, ident):
    outs, mids = grid.outers, grid.mids
    dma = pltpu.SemaphoreType.DMA
    many, steps, pair = max(mids - 1, 1), max(outs - 1, 1), max(grid.n_dp - 1, 1)
    scratch, shapes = [], []
    for term, count in zip(terms, counts):
        rows, part = term.shape[1:]
        shapes.append(jax.ShapeDtypeStruct((grid.n_dp, count, part), jnp.bfloat16))
        scratch += [
            pltpu.VMEM((mids, outs, rows, part), jnp.float32),
            pltpu.VMEM((many, outs, rows, part), jnp.bfloat16),
            pltpu.VMEM((many, outs, rows, part), jnp.bfloat16),
            pltpu.VMEM((steps, rows, part), jnp.bfloat16),
            pltpu.VMEM((steps, rows, part), jnp.bfloat16),
            pltpu.VMEM((grid.n_dp, count, part), jnp.bfloat16),
            dma((mids, outs)), dma((mids, outs)),
            dma((many, outs)), dma((many, outs)),
            dma((steps,)), dma((steps,)),
            dma((pair,)), dma((pair,)),
        ]
    results = pl.pallas_call(
        functools.partial(scatter_kernel, grid, counts),
        out_shape=shapes,
        in_specs=vmem(len(terms)),
        out_specs=vmem(len(terms)),
        scratch_shapes=scratch,
        compiler_params=pltpu.CompilerParams(
            collective_id=ident, has_side_effects=True, vmem_limit_bytes=VMEM_LIMIT
        ),
        cost_estimate=pl.CostEstimate(flops=0, bytes_accessed=60_000_000, transcendentals=0),
        name="scatter_sums",
    )(*terms)
    return [
        result.transpose(1, 0, 2).reshape(result.shape[1], -1) for result in results
    ]


def shifted(value, n_dp, step):
    return lax.ppermute(value, "dp", [(i, (i + step) % n_dp) for i in range(n_dp)])


def all_parts(value, n_dp):
    dp = lax.axis_index("dp")
    stacked = jnp.stack([value] + [shifted(value, n_dp, s) for s in range(1, n_dp)])
    return jnp.stack([
        lax.dynamic_index_in_dim(stacked, lax.rem(dp - n + n_dp, n_dp), 0, keepdims=False) for n in range(n_dp)
    ])


def exchanged(part, kind, n_dp):
    sent = part.astype(kind)
    return [shifted(sent, n_dp, s) for s in range(1, n_dp)]


def total_of(part, others):
    for other in others:
        part = part + other.astype(jnp.float32)
    return part


CHUNKS = 2


def per_device(
    grid, hidden, targets, loss_weight, head_weight, gate_weight, up_weight, down_trans,
    block_input, block_cotangent,
):
    n_dp, n_vocab = grid.n_dp, grid.n_vocab
    rows, rows_b = hidden.shape[0], block_input.shape[0]
    part = head_weight.shape[0]

    def ordered(value):
        return all_parts(value, n_dp).reshape(n_dp, n_vocab, rows).transpose(1, 0, 2).reshape(-1)

    both = jnp.concatenate([block_input, block_cotangent], axis=0)
    head_rows, both_part = gather_rows(grid, split_features(grid, hidden), split_features(grid, both), 1)
    targets_all, weight_all = ordered(targets), ordered(loss_weight)
    local_target = targets_all - lax.axis_index("vocab") * head_weight.shape[1]

    chunk = n_vocab // CHUNKS
    parts, others = [], []
    for c in range(CHUNKS):
        chunk_rows = head_rows[c * chunk:(c + 1) * chunk].reshape(-1, part)
        if c:
            chunk_rows, _ = lax.optimization_barrier((chunk_rows, parts[-1]))
        product = jnp.dot(chunk_rows, head_weight, preferred_element_type=jnp.float32)
        sent = product.astype(jnp.float16)
        parts.append(product)
        others.append([shifted(sent, n_dp, s) for s in range(1, n_dp)])
    both_part, _ = lax.optimization_barrier((both_part, parts[-1]))

    both_all, = gather_rows(grid, both_part, None, 2)
    in_rows = both_all[:, :, :rows_b].reshape(-1, part)
    cot_rows = both_all[:, :, rows_b:].reshape(-1, part)
    gate_part = jnp.dot(in_rows, gate_weight, preferred_element_type=jnp.float32)
    up_part = jnp.dot(in_rows, up_weight, preferred_element_type=jnp.float32)
    cot_part = jnp.dot(cot_rows, down_trans, preferred_element_type=jnp.float32)
    gate_others = exchanged(gate_part, jnp.bfloat16, n_dp)
    up_others = exchanged(up_part, jnp.bfloat16, n_dp)
    cot_others = exchanged(cot_part, jnp.bfloat16, n_dp)

    scaled, masks, totals, hits, slopes = [], [], [], [], []
    for c in range(CHUNKS):
        logits = total_of(parts[c], others[c])
        squash = jnp.tanh(logits / SOFTCAP)
        capped = SOFTCAP * squash
        cap_slope = 1.0 - squash * squash
        exponent = jnp.exp(capped)
        columns = lax.broadcasted_iota(jnp.int32, logits.shape, 1)
        size = logits.shape[0]
        mask = columns == local_target[c * size:(c + 1) * size, None]
        scaled.append(exponent * cap_slope)
        masks.append(mask)
        totals.append(jnp.sum(exponent, axis=1))
        hits.append(jnp.sum(jnp.where(mask, capped, 0.0), axis=1))
        slopes.append(jnp.sum(jnp.where(mask, cap_slope, 0.0), axis=1))
    scaled, totals, hits, slopes = lax.optimization_barrier((scaled, totals, hits, slopes))
    stats = jnp.concatenate(totals + hits).reshape(-1, 128)
    stats_sum = jnp.sum(gather_stats(grid, stats, 3), axis=0).reshape(2, -1)
    exp_total, target_logit = stats_sum[0], stats_sum[1]
    share = weight_all / exp_total
    target_share = weight_all * jnp.concatenate(slopes)
    head_terms = []
    for c in range(CHUNKS):
        size = scaled[c].shape[0]
        span = slice(c * size, (c + 1) * size)
        logit_cot = (
            share[span, None] * scaled[c] - jnp.where(masks[c], target_share[span, None], 0.0)
        ).astype(jnp.bfloat16)
        head_terms.append(right_product(logit_cot, head_weight).reshape(chunk, n_dp * rows, part))
    loss_all = (jnp.log(exp_total) - target_logit).reshape(n_vocab, n_dp, rows)
    token_loss = lax.dynamic_index_in_dim(loss_all, lax.axis_index("dp"), 1, keepdims=False).reshape(-1)
    head_terms = jnp.concatenate(head_terms, axis=0)

    gate_others, up_others, cot_others, head_terms = lax.optimization_barrier(
        (gate_others, up_others, cot_others, head_terms)
    )
    gate_pre = total_of(gate_part, gate_others)
    up_pre = total_of(up_part, up_others)
    hidden_cot = total_of(cot_part, cot_others)
    gate_act, derive = gelu_parts(gate_pre)
    gate_cot = (hidden_cot * up_pre * derive).astype(jnp.bfloat16)
    up_cot = (hidden_cot * gate_act).astype(jnp.bfloat16)
    block_terms = right_product(gate_cot, gate_weight) + right_product(up_cot, up_weight)
    block_terms = block_terms.reshape(n_vocab, n_dp * rows_b, part)
    head_out, block_out = scatter_sums(grid, (head_terms, block_terms), (rows, rows_b), 4)
    return (token_loss, head_out, block_out)


def solution(mesh):
    grid = Grid(mesh.shape["dp"], mesh.shape["vocab"])
    return jax.shard_map(
        functools.partial(per_device, grid),
        mesh=mesh,
        in_specs=(
            P(("dp", "vocab"), None),
            P("dp"),
            P("dp"),
            P("dp", "vocab"),
            P("dp", "vocab"),
            P("dp", "vocab"),
            P("dp", "vocab"),
            P(("dp", "vocab"), None),
            P(("dp", "vocab"), None),
        ),
        out_specs=(P("dp"), P(("dp", "vocab"), None), P(("dp", "vocab"), None)),
        check_vma=False,
    )
```
